32 devices in a mesh: dp: 1 (over z), tp: 32 (over y, x, core).
Axes of the slice: x: 4, y: 4, z: 1, core: 2. Of those that a mesh axis runs over, the one named last changes fastest.
The devices are a block of a 4x4x8 slice.
Arguments:
- hidden: bfloat16 [1536, 896], P(('dp', 'tp'))
- ln_gamma: float32 [896], replicated
- ln_beta: float32 [896], replicated
- out_embed: bfloat16 [155648, 896], P('tp')
- vocab_valid: int32 [155648], P('tp')
- targets: int32 [1536], P(('dp', 'tp'))
- loss_mask: int32 [1536], P(('dp', 'tp'))
Outputs:
- output 1: float32 [1536], P(('dp', 'tp'))
- output 2: float32 [1], P('dp')
- output 3: bfloat16 [1536, 896], P(('dp', 'tp'))
- output 4: float32 [155648, 896], P(('dp', 'tp'))
- output 5: float32 [896], P('dp')
- output 6: float32 [896], P('dp')
All inputs are finite; a program needn't handle non-finite values.
Results may differ from the reference program's by a relative error of at most 0.001.
Values are sent between devices in bfloat16 or wider.
A program may use at most 768 MiB of HBM per device.

```python
import jax
import jax.numpy as jnp
from jax import lax

GROUP_SIZE = 32
TOKENS_DEV = 48
MODEL_DIM = 896
VOCAB_SIZE = 151936

SEQ_LEN = GROUP_SIZE * TOKENS_DEV
PAD_UNIT = 128 * GROUP_SIZE
VOCAB_PAD = (VOCAB_SIZE + PAD_UNIT - 1) // PAD_UNIT * PAD_UNIT
SHARD_VOCAB = VOCAB_PAD // GROUP_SIZE
DROP_COUNT = VOCAB_SIZE // 8
LN_EPS = 1e-5


def setup_inputs(seed: int = 0, part: int = 0) -> dict:
    base_key = jax.random.key(seed)
    k_gamma, k_beta, k_embed, k_perm = jax.random.split(base_key, 4)
    k_hidden, k_start, k_end, k_keep, k_target = jax.random.split(jax.random.fold_in(base_key, part), 5)
    hidden = jax.random.normal(k_hidden, (SEQ_LEN, MODEL_DIM), jnp.float32).astype(jnp.bfloat16)
    ln_gamma = 1.0 + 0.3 * jax.random.normal(k_gamma, (MODEL_DIM,), jnp.float32)
    ln_beta = 0.3 * jax.random.normal(k_beta, (MODEL_DIM,), jnp.float32)
    embed_scale = 2.5 * MODEL_DIM ** -0.5
    out_embed = (embed_scale * jax.random.normal(k_embed, (VOCAB_PAD, MODEL_DIM), jnp.float32)).astype(jnp.bfloat16)
    perm_ids = jax.random.permutation(k_perm, VOCAB_SIZE)
    vocab_ids = jnp.arange(VOCAB_PAD)
    vocab_valid = (vocab_ids < VOCAB_SIZE).astype(jnp.int32).at[perm_ids[:DROP_COUNT]].set(0)
    allowed_ids = perm_ids[DROP_COUNT:]
    pick_idx = jax.random.randint(k_target, (SEQ_LEN,), 0, VOCAB_SIZE - DROP_COUNT)
    targets = allowed_ids[pick_idx].astype(jnp.int32)
    positions = jnp.arange(SEQ_LEN)
    half_shard = TOKENS_DEV // 2
    start_pos = jax.random.randint(k_start, (), 0, half_shard + 1)
    end_pos = SEQ_LEN - jax.random.randint(k_end, (), 0, half_shard + 1)
    keep_tok = (jax.random.randint(k_keep, (SEQ_LEN,), 0, 4) != 0) | (positions == SEQ_LEN // 2)
    loss_mask = ((positions >= start_pos) & (positions < end_pos) & keep_tok).astype(jnp.int32)
    return {"hidden": hidden, "ln_gamma": ln_gamma, "ln_beta": ln_beta, "out_embed": out_embed, "vocab_valid": vocab_valid, "targets": targets, "loss_mask": loss_mask}


def layer_norm(hidden32, ln_gamma, ln_beta):
    row_mean = jnp.mean(hidden32, axis=-1, keepdims=True)
    centered = hidden32 - row_mean
    row_var = jnp.mean(centered * centered, axis=-1, keepdims=True)
    return centered * lax.rsqrt(row_var + LN_EPS) * ln_gamma + ln_beta


def reference(hidden, ln_gamma, ln_beta, out_embed, vocab_valid, targets, loss_mask):
    normed, ln_vjp = jax.vjp(layer_norm, hidden.astype(jnp.float32), ln_gamma, ln_beta)
    x_all = normed.astype(jnp.bfloat16)
    allowed = vocab_valid[None, :] > 0
    vocab_ids = jnp.arange(VOCAB_PAD)
    x_blocks = x_all.reshape(GROUP_SIZE, TOKENS_DEV, MODEL_DIM)
    tgt_blocks = targets.reshape(GROUP_SIZE, TOKENS_DEV)

    def token_block(block_args):
        x_blk, tgt_blk = block_args
        logits = jnp.dot(x_blk, out_embed.T, preferred_element_type=jnp.float32)
        log_norm = jax.nn.logsumexp(jnp.where(allowed, logits, -jnp.inf), axis=-1)
        picked = jnp.sum(jnp.where(vocab_ids[None, :] == tgt_blk[:, None], logits, 0.0), axis=-1)
        return log_norm, picked

    log_norm, picked = lax.map(token_block, (x_blocks, tgt_blocks))
    log_norm = log_norm.reshape(SEQ_LEN)
    picked = picked.reshape(SEQ_LEN)
    weight = loss_mask.astype(jnp.float32)
    tok_count = jnp.sum(weight)
    tok_loss = (log_norm - picked) * weight
    mean_loss = jnp.sum(tok_loss) / tok_count
    tok_scale = weight / tok_count

    embed_shards = out_embed.reshape(GROUP_SIZE, SHARD_VOCAB, MODEL_DIM)
    valid_shards = vocab_valid.reshape(GROUP_SIZE, SHARD_VOCAB)
    shard_start = jnp.arange(GROUP_SIZE) * SHARD_VOCAB

    def vocab_block(dx_acc, block_args):
        emb_blk, valid_blk, offset = block_args
        logits = jnp.dot(x_all, emb_blk.T, preferred_element_type=jnp.float32)
        soft_probs = jnp.where(valid_blk[None, :] > 0, jnp.exp(logits - log_norm[:, None]), 0.0)
        target_hit = (offset + jnp.arange(SHARD_VOCAB))[None, :] == targets[:, None]
        d_logits = ((soft_probs - target_hit.astype(jnp.float32)) * tok_scale[:, None]).astype(jnp.bfloat16)
        d_emb = jnp.dot(d_logits.T, x_all, preferred_element_type=jnp.float32)
        dx_acc = dx_acc + jnp.dot(d_logits, emb_blk, preferred_element_type=jnp.float32)
        return dx_acc, d_emb

    dx_all, d_embed = lax.scan(vocab_block, jnp.zeros((SEQ_LEN, MODEL_DIM), jnp.float32), (embed_shards, valid_shards, shard_start))
    d_embed = d_embed.reshape(VOCAB_PAD, MODEL_DIM)
    d_hidden, d_gamma, d_beta = ln_vjp(dx_all)
    return tok_loss, mean_loss.reshape(1), d_hidden.astype(jnp.bfloat16), d_embed, d_gamma, d_beta
```

```python
import functools
import math

import jax
import jax.numpy as jnp
from jax import lax
from jax.experimental import pallas as pl
from jax.experimental.pallas import tpu as pltpu
from jax.sharding import PartitionSpec as P

LN_EPS = 1e-5
F32 = jnp.float32
BF16 = jnp.bfloat16
LANES = 128
LOW = -3e38
NN = (((1,), (0,)), ((), ()))
NT = (((1,), (1,)), ((), ()))
TN = (((0,), (0,)), ((), ()))


def dot(a, b, dims):
    return lax.dot_general(a, b, dims, preferred_element_type=F32)


def pieces(lo, hi, size):
    return [(o, min(size, hi - o)) for o in range(lo, hi, size)]


def head_kernel(
    side, tok, dim, vocab,
    hid_ref, gamma_ref, beta_ref, aux_ref, bias_ref, emb_hbm,
    loss_ref, mean_ref, dhid_ref, dln_ref, dz_hbm, x_hbm,
    emb, xbuf, z, tcol, stage, ms, ss, pk, lsec, wcol,
    st, rowa, rowb, mrow, lrow,
    dxt, rca, rcb, rcd, rcc, ga, gb, gpart,
    emb_sem, ag_s, ag_r, sa_s, sa_r, sb_s, sb_r,
    s0_s, s0_r, s1_s, s1_r, s2_s, s2_r, s3_s, s3_r,
    ga_s, ga_r, gb_s, gb_r, dz_sem, x_sem,
):
    n_row = 2 * side
    wide = dim + LANES
    me = lax.axis_index("tp")
    c = lax.rem(me, 2)
    x = lax.rem(me // 2, side)
    y = me // n_row
    off = me * vocab

    def wrap(v):
        return lax.rem(v + 4 * side, side)

    def dev(yy, xx, cc):
        return {"tp": (wrap(yy) * side + wrap(xx)) * 2 + cc}

    right, left = dev(y, x + 1, c), dev(y, x - 1, c)
    up, down = dev(y - 1, x, c), dev(y + 1, x, c)
    partner = dev(y, x, 1 - c)
    row_peers = [(dx, h) for h in range(2) for dx in range(side) if (dx, h) != (0, 0)]

    def other(h):
        return c if h == 0 else 1 - c

    def remote(src, dst, s, r, to):
        return pltpu.make_async_remote_copy(
            src_ref=src, dst_ref=dst, send_sem=s, recv_sem=r,
            device_id=to, device_id_type=pl.DeviceIdType.MESH)

    emb_copy = pltpu.make_async_copy(emb_hbm, emb, emb_sem)
    emb_copy.start()

    barrier = pltpu.get_barrier_semaphore()
    for dx, h in row_peers:
        pl.semaphore_signal(barrier, inc=1, device_id=dev(y, x + dx, other(h)),
                            device_id_type=pl.DeviceIdType.MESH)
    for dy in range(1, side):
        pl.semaphore_signal(barrier, inc=1, device_id=dev(y + dy, x, c),
                            device_id_type=pl.DeviceIdType.MESH)

    def normed():
        h32 = hid_ref[...].astype(F32)
        cen = h32 - jnp.mean(h32, axis=-1, keepdims=True)
        rstd = lax.rsqrt(jnp.mean(cen * cen, axis=-1, keepdims=True) + LN_EPS)
        return cen * rstd, rstd

    xhat0, _ = normed()
    xbuf[0, :, 0:dim] = (xhat0 * gamma_ref[...] + beta_ref[...]).astype(BF16)
    xbuf[0, :, dim:wide] = aux_ref[...]
    pl.semaphore_wait(barrier, len(row_peers) + side - 1)

    cut = 2 * tok // 3
    lo, hi = pl.ds(0, cut), pl.ds(cut, tok - cut)
    ag_ops = {}

    def ag(k, src, dst, to, rows=None):
        a, b = xbuf.at[src], xbuf.at[dst]
        if rows is not None:
            a, b = xbuf.at[src, rows], xbuf.at[dst, rows]
        ag_ops[k] = remote(a, b, ag_s.at[k], ag_r.at[k], to)
        ag_ops[k].start()

    ag(0, 0, 3, right)
    ag(1, 0, 1, left)
    ag(2, 0, 4, partner)
    ag(3, 0, 8, up)
    ag(4, 0, 24, down)
    ag_ops[0].wait_recv()
    ag(5, 3, 2, right, lo)
    ag(7, 3, 7, partner)
    ag(9, 3, 11, up)
    ag(10, 3, 27, down)
    ag_ops[1].wait_recv()
    ag(6, 1, 2, left, hi)
    ag(8, 1, 5, partner)
    ag(11, 1, 9, up)
    ag(12, 1, 25, down)
    ag_ops[5].wait_recv()
    ag_ops[6].wait_recv()
    ag(13, 2, 6, partner)
    ag(14, 2, 10, up)
    ag(15, 2, 26, down)
    for k in (2, 7, 8, 13):
        ag_ops[k].wait_recv()
    for k, src, dst, to in ((16, (8, 4), (12, 4), partner), (17, (24, 4), (28, 4), partner),
                            (18, (8, 2), (16, 2), up), (19, (26, 2), (18, 2), down),
                            (20, (16, 4), (20, 4), partner)):
        ag_ops[k] = remote(xbuf.at[pl.ds(*src)], xbuf.at[pl.ds(*dst)], ag_s.at[k], ag_r.at[k], to)

    def row_of(t):
        return wrap(y + t)

    def sa_op(t, d):
        dx, h = row_peers[d]
        r = row_of(t)
        return remote(st.at[r, pl.ds(0, 3)], rowa.at[t, 2 * x + c], sa_s.at[t, d], sa_r.at[t, d],
                      dev(y, x + dx, other(h)))

    def sa_wait(t, d):
        dx, h = row_peers[d]
        slot = 2 * wrap(x - dx) + other(h)
        remote(rowa.at[t, slot], rowa.at[t, slot], sa_s.at[t, d], sa_r.at[t, d], partner).wait_recv()

    def sb_op(t, dy):
        r = row_of(t)
        return remote(rowb.at[r, y], rowb.at[r, y], sb_s.at[t, dy], sb_r.at[t, dy], dev(y + dy, x, c))

    def sb_wait(t, dy):
        yy = wrap(y - dy)
        ref = rowb.at[wrap(yy + t), yy]
        remote(ref, ref, sb_s.at[t, dy], sb_r.at[t, dy], partner).wait_recv()

    def merge(parts):
        m = functools.reduce(jnp.maximum, [p[0] for p in parts])
        s = functools.reduce(jnp.add, [p[1] * jnp.exp(p[0] - m) for p in parts])
        return m, s, functools.reduce(jnp.add, [p[2] for p in parts])

    def row_merge(t):
        for d in range(len(row_peers)):
            sa_wait(t, d)
        m, s, q = merge([[rowa[t, i, k] for k in range(3)] for i in range(n_row)])
        r = row_of(t)
        rowb[r, y, 0] = m
        rowb[r, y, 1] = s
        rowb[r, y, 2] = q
        for dy in range(1, side):
            sb_op(t, dy).start()

    half = (vocab // LANES // 2) * LANES
    lane = lax.broadcasted_iota(jnp.int32, (tok, LANES), 1)
    digit = jnp.where(lane == 0, 1.0, jnp.where(lane == 1, 256.0, jnp.where(lane == 2, 65536.0, 0.0)))

    def logits_tile(t, carry):
        @pl.when(t == 1)
        def _():
            ag_ops[16].wait_recv()

        @pl.when(t == 2)
        def _():
            ag_ops[20].wait_recv()

        @pl.when(t == 3)
        def _():
            ag_ops[17].wait_recv()

        base = 8 * t
        for p in range(8):
            code = jnp.sum(xbuf[base + p, :, dim:wide].astype(F32) * digit, axis=1, keepdims=True)
            tcol[base + p] = jnp.broadcast_to(code.astype(jnp.int32) - 1 - off, (tok, LANES))
        ms[...] = jnp.full(ms.shape, LOW, F32)
        ss[...] = jnp.zeros(ss.shape, F32)
        pk[...] = jnp.zeros(pk.shape, F32)

        def do_dot(o, n):
            xt = xbuf[pl.ds(base, 8), :, 0:dim].reshape(8 * tok, dim)
            r = dot(xt, emb[o:o + n, :], NT) + bias_ref[:, o:o + n]
            z[pl.ds(base, 8), :, o:o + n] = r.reshape(8, tok, n)

        def do_stats(o, n):
            for p in range(8):
                m0, tl, q = ms[p], tcol[base + p], pk[p]
                zs = [z[base + p, :, o + i:o + i + LANES] for i in range(0, n, LANES)]
                m1 = functools.reduce(jnp.maximum, zs, m0)
                s = ss[p] * jnp.exp(m0 - m1)
                for i, v in enumerate(zs):
                    s = s + jnp.exp(v - m1)
                    q = q + jnp.where(lane + (o + i * LANES) == tl, v, 0.0)
                ms[p], ss[p], pk[p] = m1, s, q

        def run(lo_, hi_):
            cs = pieces(lo_, hi_, 512)
            do_dot(*cs[0])
            for a, b in zip(cs[1:], cs[:-1]):
                do_dot(*a)
                do_stats(*b)
            do_stats(*cs[-1])

        run(0, half)

        @pl.when(t == 0)
        def _():
            for k in (3, 9, 11, 14):
                ag_ops[k].wait_recv()
            ag_ops[16].start()
            ag_ops[18].start()
            for k in (4, 10, 12, 15):
                ag_ops[k].wait_recv()
            ag_ops[17].start()
            ag_ops[19].start()

        @pl.when(t == 1)
        def _():
            ag_ops[18].wait_recv()
            ag_ops[19].wait_recv()
            ag_ops[20].start()

        @pl.when(t > 0)
        def _():
            row_merge(t - 1)

        run(half, vocab)

        r = row_of(t)
        for p in range(8):
            h, j = p // 4, p % 4
            m1 = jnp.max(ms[p], axis=1, keepdims=True)
            s1 = jnp.sum(ss[p] * jnp.exp(ms[p] - m1), axis=1, keepdims=True)
            q1 = jnp.sum(pk[p], axis=1, keepdims=True)
            live = jnp.where(tcol[base + p] == -1 - off, 0.0, 1.0)
            packed = jnp.where(lane == 0, m1, jnp.where(lane == 1, s1, jnp.where(lane == 2, q1, live)))
            flat = jnp.concatenate([packed, jnp.zeros((LANES - tok, LANES), F32)], axis=0).T
            sub = 2 * wrap(x + j) + other(h)
            for k in range(3):
                st[r, k, pl.ds(sub, 1), :] = flat[k:k + 1, :]
            mrow[r, pl.ds(sub, 1), :] = flat[3:4, :]
        for k in range(3):
            rowa[t, 2 * x + c, k] = st[r, k]
        for d in range(len(row_peers)):
            sa_op(t, d).start()
        return carry

    emb_copy.wait()
    lax.fori_loop(0, side, logits_tile, 0)
    row_merge(side - 1)
    for t in range(side):
        for dy in range(1, side):
            sb_wait(t, dy)

    n_tok = jnp.sum(mrow[...])
    inv_n = 1.0 / n_tok
    total = jnp.zeros((n_row, LANES), F32)
    lanes8 = lax.broadcasted_iota(jnp.int32, (n_row, LANES), 1)
    for r in range(side):
        m, s, q = merge([[rowb[r, i, k] for k in range(3)] for i in range(side)])
        lse = m + jnp.log(s)
        lrow[r] = lse
        tl = jnp.where(lanes8 < tok, (lse - q) * mrow[r], 0.0)
        st[r, 3] = tl
        total = total + tl
    loss_ref[...] = st[y, 3, pl.ds(2 * x + c, 1), :]
    mean_ref[...] = jnp.broadcast_to(jnp.sum(total) / n_tok, (1, LANES))

    def blk(k, p):
        h, j = p // 4, p % 4
        cc = other(h)
        yy = wrap(jnp.where(cc == 0, x + j + k, y + j))
        xx = wrap(jnp.where(cc == 0, x + j, y + j - k))
        pos = 8 * wrap(yy - y) + 4 * h + wrap(xx - x)
        return pos, yy, 2 * xx + cc

    along = c
    nxt = dev(y + along, x + 1 - along, c)
    prv = dev(y - along, x - 1 + along, c)
    top, bot = pl.ds(0, tok // 2), pl.ds(tok // 2, tok - tok // 2)

    def s0(k):
        return remote(dxt.at[k, pl.ds(4, 4)], rca.at[k], s0_s.at[k], s0_r.at[k], partner)

    def s1(k, d):
        src = dxt.at[k, 2, top] if d == 0 else dxt.at[k, 2, bot]
        return remote(src, rcb.at[k, d], s1_s.at[k, d], s1_r.at[k, d], prv if d == 0 else nxt)

    def s2(k, d):
        src = dxt.at[k, 1] if d == 0 else dxt.at[k, 3]
        return remote(src, rcd.at[k, d], s2_s.at[k, d], s2_r.at[k, d], nxt if d == 0 else prv)

    def s3_far(k):
        return wrap(jnp.where(c == 0, x + k - y, y - k - x))

    def s3(k):
        i = s3_far(k)
        to = dev(jnp.where(c == 0, x + k, y), jnp.where(c == 0, x, y - k), c)
        slot = wrap(side - i)
        return remote(dxt.at[k, 0], rcc.at[slot], s3_s.at[k], s3_r.at[slot], to)

    def do_s1(k):
        s0(k).wait_recv()
        for j in range(4):
            dxt[k, j] = dxt[k, j] + rca[k, j]
        s1(k, 0).start()
        s1(k, 1).start()

    def do_s2(k):
        s1(k, 0).wait_recv()
        s1(k, 1).wait_recv()
        n = tok // 2
        dxt[k, 3, 0:n] = dxt[k, 3, 0:n] + rcb[k, 0]
        dxt[k, 1, n:tok] = dxt[k, 1, n:tok] + rcb[k, 1]
        s2(k, 0).start()
        s2(k, 1).start()

    def do_s3(k):
        s2(k, 0).wait_recv()
        s2(k, 1).wait_recv()
        dxt[k, 0] = dxt[k, 0] + rcd[k, 0] + rcd[k, 1]
        i = s3_far(k)

        @pl.when(i != 0)
        def _():
            s3(k).start()

        @pl.when(i == 0)
        def _():
            rcc[0] = dxt[k, 0]

    def dz_out(k):
        return pltpu.make_async_copy(
            stage.at[lax.rem(k, 2)], dz_hbm.at[pl.ds(pl.multiple_of(k * 8 * tok, 8 * tok), 8 * tok)], dz_sem.at[k])

    def x_out(k, p):
        pos, _, _ = blk(k, p)
        return pltpu.make_async_copy(
            xbuf.at[pos, :, pl.ds(0, dim)],
            x_hbm.at[pl.ds(pl.multiple_of((8 * k + p) * tok, 16), tok)], x_sem.at[8 * k + p])

    def grad_tile(k, carry):
        where = [blk(k, p) for p in range(8)]
        for p, (pos, yy, sub) in enumerate(where):
            row = lrow[yy, pl.ds(sub, 1), :]
            lsec[p] = jnp.broadcast_to(row, (LANES, LANES)).T[0:tok, :]
            wcol[p] = jnp.where(tcol[pos] == -1 - off, 0.0, inv_n)
            x_out(k, p).start()
        buf = lax.rem(k, 2)

        @pl.when(k >= 2)
        def _():
            dz_out(k - 2).wait()

        def part(o, n):
            rows = []
            for p, (pos, _, _) in enumerate(where):
                l, w, tl = lsec[p], wcol[p], tcol[pos]
                cols = []
                for i in range(o, o + n, LANES):
                    e = jnp.exp(z[pos, :, i:i + LANES] - l)
                    e = jnp.where(lane + i == tl, e - 1.0, e) * w
                    cols.append(e.astype(BF16))
                rows.append(jnp.concatenate(cols, axis=1))
            dz = jnp.concatenate(rows, axis=0)
            stage[buf, :, o:o + n] = dz
            return dot(dz, emb[o:o + n, :], NN)

        def span(lo_, hi_):
            return functools.reduce(jnp.add, [part(o, n) for o, n in pieces(lo_, hi_, 512)])

        dxt[k] = span(0, half).reshape(8, tok, dim)

        @pl.when(k >= 1)
        def _():
            do_s1(k - 1)

        @pl.when(k >= 2)
        def _():
            do_s2(k - 2)

        @pl.when(k >= 3)
        def _():
            do_s3(k - 3)

        dxt[k] = dxt[k] + span(half, vocab).reshape(8, tok, dim)
        s0(k).start()
        dz_out(k).start()
        return carry

    lax.fori_loop(0, side, grad_tile, 0)
    last = side - 1
    do_s1(last)
    do_s2(last - 1)
    do_s3(last - 2)
    do_s2(last)
    do_s3(last - 1)
    do_s3(last)
    for i in range(1, side):
        ref = rcc.at[i]
        remote(ref, ref, s3_s.at[0], s3_r.at[i], partner).wait_recv()

    dx = rcc[0] + rcc[1] + rcc[2] + rcc[3]
    xhat, rstd = normed()
    g = dx * gamma_ref[...]
    dh = rstd * (g - jnp.mean(g, axis=-1, keepdims=True) - xhat * jnp.mean(g * xhat, axis=-1, keepdims=True))
    gpart[0:1, :] = jnp.sum(dx * xhat, axis=0, keepdims=True)
    gpart[1:2, :] = jnp.sum(dx, axis=0, keepdims=True)

    def ga_op(d):
        ddx, h = row_peers[d]
        return remote(gpart, ga.at[2 * x + c], ga_s.at[d], ga_r.at[d], dev(y, x + ddx, other(h)))

    def gb_op(dy):
        return remote(gb.at[y], gb.at[y], gb_s.at[dy], gb_r.at[dy], dev(y + dy, x, c))

    for d in range(len(row_peers)):
        ga_op(d).start()
    dhid_ref[...] = dh.astype(BF16)
    ga[2 * x + c] = gpart[...]
    for d, (ddx, h) in enumerate(row_peers):
        ref = ga.at[2 * wrap(x - ddx) + other(h)]
        remote(ref, ref, ga_s.at[d], ga_r.at[d], partner).wait_recv()
    gb[y] = functools.reduce(jnp.add, [ga[i] for i in range(n_row)])
    for dy in range(1, side):
        gb_op(dy).start()
    for dy in range(1, side):
        ref = gb.at[wrap(y - dy)]
        remote(ref, ref, gb_s.at[dy], gb_r.at[dy], partner).wait_recv()
    dln_ref[...] = functools.reduce(jnp.add, [gb[i] for i in range(side)])

    for k in sorted(ag_ops):
        ag_ops[k].wait_send()
    for t in range(side):
        for d in range(len(row_peers)):
            sa_op(t, d).wait_send()
        for dy in range(1, side):
            sb_op(t, dy).wait_send()
        s0(t).wait_send()
        for d in range(2):
            s1(t, d).wait_send()
            s2(t, d).wait_send()

        @pl.when(s3_far(t) != 0)
        def _():
            s3(t).wait_send()

        for p in range(8):
            x_out(t, p).wait()
    for d in range(len(row_peers)):
        ga_op(d).wait_send()
    for dy in range(1, side):
        gb_op(dy).wait_send()
    dz_out(side - 2).wait()
    dz_out(side - 1).wait()


def head(mesh, hid, gamma, beta, aux, bias, emb):
    n_dev = mesh.shape["tp"]
    side = math.isqrt(n_dev // 2)
    tok, dim = hid.shape
    vocab = emb.shape[0]
    seq = tok * n_dev
    n_row = 2 * side
    vmem = pl.BlockSpec(memory_space=pltpu.VMEM)
    hbm = pl.BlockSpec(memory_space=pl.ANY)
    dma = pltpu.SemaphoreType.DMA
    return pl.pallas_call(
        functools.partial(head_kernel, side, tok, dim, vocab),
        out_shape=(
            jax.ShapeDtypeStruct((1, LANES), F32),
            jax.ShapeDtypeStruct((1, LANES), F32),
            jax.ShapeDtypeStruct((tok, dim), BF16),
            jax.ShapeDtypeStruct((2, dim), F32),
            jax.ShapeDtypeStruct((seq, vocab), BF16),
            jax.ShapeDtypeStruct((seq, dim), BF16),
        ),
        in_specs=[vmem] * 5 + [hbm],
        out_specs=(vmem, vmem, vmem, vmem, hbm, hbm),
        scratch_shapes=[
            pltpu.VMEM((vocab, dim), BF16),
            pltpu.VMEM((n_dev, tok, dim + LANES), BF16),
            pltpu.VMEM((n_dev, tok, vocab), F32),
            pltpu.VMEM((n_dev, tok, LANES), jnp.int32),
            pltpu.VMEM((2, 8 * tok, vocab), BF16),
            pltpu.VMEM((8, tok, LANES), F32),
            pltpu.VMEM((8, tok, LANES), F32),
            pltpu.VMEM((8, tok, LANES), F32),
            pltpu.VMEM((8, tok, LANES), F32),
            pltpu.VMEM((8, tok, LANES), F32),
            pltpu.VMEM((side, 4, n_row, LANES), F32),
            pltpu.VMEM((side, n_row, 3, n_row, LANES), F32),
            pltpu.VMEM((side, side, 3, n_row, LANES), F32),
            pltpu.VMEM((side, n_row, LANES), F32),
            pltpu.VMEM((side, n_row, LANES), F32),
            pltpu.VMEM((side, 8, tok, dim), F32),
            pltpu.VMEM((side, 4, tok, dim), F32),
            pltpu.VMEM((side, 2, tok // 2, dim), F32),
            pltpu.VMEM((side, 2, tok, dim), F32),
            pltpu.VMEM((side, tok, dim), F32),
            pltpu.VMEM((n_row, 2, dim), F32),
            pltpu.VMEM((side, 2, dim), F32),
            pltpu.VMEM((2, dim), F32),
            dma,
            dma((21,)), dma((21,)),
            dma((side, n_row - 1)), dma((side, n_row - 1)),
            dma((side, side)), dma((side, side)),
            dma((side,)), dma((side,)),
            dma((side, 2)), dma((side, 2)),
            dma((side, 2)), dma((side, 2)),
            dma((side,)), dma((side,)),
            dma((n_row - 1,)), dma((n_row - 1,)),
            dma((side,)), dma((side,)),
            dma((side,)), dma((n_dev,)),
        ],
        compiler_params=pltpu.CompilerParams(
            collective_id=0, has_side_effects=True, vmem_limit_bytes=67043328),
        name="head",
    )(hid, gamma, beta, aux, bias, emb)


def dembed_kernel(x_ref, dz_ref, out_ref):
    out_ref[...] = dot(dz_ref[...], x_ref[...], TN)


def dembed(x, dz):
    seq, dim = x.shape
    vocab = dz.shape[1]
    cols = 1664
    return pl.pallas_call(
        dembed_kernel,
        out_shape=jax.ShapeDtypeStruct((vocab, dim), F32),
        grid=(pl.cdiv(vocab, cols),),
        in_specs=[pl.BlockSpec((seq, dim), lambda i: (0, 0)), pl.BlockSpec((seq, cols), lambda i: (0, i))],
        out_specs=pl.BlockSpec((cols, dim), lambda i: (i, 0)),
        compiler_params=pltpu.CompilerParams(vmem_limit_bytes=67043328),
        name="dembed",
    )(x, dz)


def solution(mesh):
    tok_spec = P(("dp", "tp"))
    row_spec = P(("dp", "tp"), None)

    def local_step(hidden_blk, ln_gamma, ln_beta, embed_blk, valid_blk, tgt_blk, mask_blk):
        tok = hidden_blk.shape[0]
        code = jnp.where(mask_blk > 0, tgt_blk + 1, 0)
        lane = lax.broadcasted_iota(jnp.int32, (tok, LANES), 1)
        aux = jnp.where(lane < 3, (code[:, None] >> (8 * jnp.minimum(lane, 2))) & 255, 0).astype(BF16)
        bias = jnp.where(valid_blk > 0, 0.0, -jnp.inf).astype(F32)[None, :]
        loss, mean, dhid, dln, dz, x = head(
            mesh, hidden_blk, ln_gamma[None, :], ln_beta[None, :], aux, bias, embed_blk)
        d_embed = dembed(x, dz)
        return loss[0, :tok], mean[0, :1], dhid, d_embed, dln[0], dln[1]

    return jax.shard_map(
        local_step, mesh=mesh,
        in_specs=(row_spec, P(), P(), P("tp", None), P("tp"), tok_spec, tok_spec),
        out_specs=(tok_spec, P("dp"), row_spec, row_spec, P("dp"), P("dp")), check_vma=False)
```

```python
import functools
import math

import jax
import jax.numpy as jnp
from jax import lax
from jax.experimental import pallas as pl
from jax.experimental.pallas import tpu as pltpu
from jax.sharding import PartitionSpec as P

LN_EPS = 1e-5
F32 = jnp.float32
BF16 = jnp.bfloat16
LANES = 128
LOW = -3e38
NN = (((1,), (0,)), ((), ()))
NT = (((1,), (1,)), ((), ()))
TN = (((0,), (0,)), ((), ()))


def dot(a, b, dims):
    return lax.dot_general(a, b, dims, preferred_element_type=F32)


def pieces(lo, hi, size):
    return [(o, min(size, hi - o)) for o in range(lo, hi, size)]


def head_kernel(
    side, tok, dim, vocab,
    hid_ref, gamma_ref, beta_ref, valid_ref, tgt_ref, mask_ref, emb_hbm,
    loss_ref, mean_ref, dhid_ref, dln_ref, dz_hbm, x_hbm,
    emb, xbuf, z, bias_ref, crow, tcol, stage, ms, ss, pk, lsec, wcol,
    st, rowa, rowb, mrow, lrow,
    dxt, rca, rcb, rcd, rcc, ga, gb, gpart,
    emb_sem, ag_s, ag_r, sa_s, sa_r, sb_s, sb_r,
    s0_s, s0_r, s1_s, s1_r, s2_s, s2_r, s3_s, s3_r,
    ga_s, ga_r, gb_s, gb_r, dz_sem, x_sem,
):
    n_row = 2 * side
    wide = dim + LANES
    me = lax.axis_index("tp")
    c = lax.rem(me, 2)
    x = lax.rem(me // 2, side)
    y = me // n_row
    off = me * vocab

    def wrap(v):
        return lax.rem(v + 4 * side, side)

    def dev(yy, xx, cc):
        return {"tp": (wrap(yy) * side + wrap(xx)) * 2 + cc}

    right, left = dev(y, x + 1, c), dev(y, x - 1, c)
    up, down = dev(y - 1, x, c), dev(y + 1, x, c)
    partner = dev(y, x, 1 - c)
    row_peers = [(dx, h) for h in range(2) for dx in range(side) if (dx, h) != (0, 0)]

    def other(h):
        return c if h == 0 else 1 - c

    def remote(src, dst, s, r, to):
        return pltpu.make_async_remote_copy(
            src_ref=src, dst_ref=dst, send_sem=s, recv_sem=r,
            device_id=to, device_id_type=pl.DeviceIdType.MESH)

    emb_copy = pltpu.make_async_copy(emb_hbm, emb, emb_sem)
    emb_copy.start()

    barrier = pltpu.get_barrier_semaphore()
    for dx, h in row_peers:
        pl.semaphore_signal(barrier, inc=1, device_id=dev(y, x + dx, other(h)),
                            device_id_type=pl.DeviceIdType.MESH)
    for dy in range(1, side):
        pl.semaphore_signal(barrier, inc=1, device_id=dev(y + dy, x, c),
                            device_id_type=pl.DeviceIdType.MESH)

    def normed():
        h32 = hid_ref[...].astype(F32)
        cen = h32 - jnp.mean(h32, axis=-1, keepdims=True)
        rstd = lax.rsqrt(jnp.mean(cen * cen, axis=-1, keepdims=True) + LN_EPS)
        return cen * rstd, rstd

    xhat0, _ = normed()
    xbuf[0, :, 0:dim] = (xhat0 * gamma_ref[...][None, :] + beta_ref[...][None, :]).astype(BF16)
    crow[...] = jnp.zeros((1, LANES), F32)
    crow[0:1, 0:tok] = jnp.where(mask_ref[...] > 0, tgt_ref[...] + 1, 0).astype(F32)[None, :]
    lane = lax.broadcasted_iota(jnp.int32, (tok, LANES), 1)
    ccol = jnp.broadcast_to(crow[...], (LANES, LANES)).T[0:tok, :].astype(jnp.int32)
    digits = jnp.where(lane == 0, ccol & 255, jnp.where(lane == 1, (ccol >> 8) & 255, (ccol >> 16) & 255))
    xbuf[0, :, dim:wide] = jnp.where(lane < 3, digits, 0).astype(F32).astype(BF16)
    pl.semaphore_wait(barrier, len(row_peers) + side - 1)

    bias_ref[...] = jnp.where(valid_ref[...] > 0, 0.0, -jnp.inf).astype(F32)[None, :]

    cut = 2 * tok // 3
    lo, hi = pl.ds(0, cut), pl.ds(cut, tok - cut)
    ag_ops = {}

    def ag(k, src, dst, to, rows=None):
        a, b = xbuf.at[src], xbuf.at[dst]
        if rows is not None:
            a, b = xbuf.at[src, rows], xbuf.at[dst, rows]
        ag_ops[k] = remote(a, b, ag_s.at[k], ag_r.at[k], to)
        ag_ops[k].start()

    ag(0, 0, 3, right)
    ag(1, 0, 1, left)
    ag(2, 0, 4, partner)
    ag(3, 0, 8, up)
    ag(4, 0, 24, down)
    ag_ops[0].wait_recv()
    ag(5, 3, 2, right, lo)
    ag(7, 3, 7, partner)
    ag(9, 3, 11, up)
    ag(10, 3, 27, down)
    ag_ops[1].wait_recv()
    ag(6, 1, 2, left, hi)
    ag(8, 1, 5, partner)
    ag(11, 1, 9, up)
    ag(12, 1, 25, down)
    ag_ops[5].wait_recv()
    ag_ops[6].wait_recv()
    ag(13, 2, 6, partner)
    ag(14, 2, 10, up)
    ag(15, 2, 26, down)
    for k in (2, 7, 8, 13):
        ag_ops[k].wait_recv()
    for k, src, dst, to in ((16, (8, 4), (12, 4), partner), (17, (24, 4), (28, 4), partner),
                            (18, (8, 2), (16, 2), up), (19, (26, 2), (18, 2), down),
                            (20, (16, 4), (20, 4), partner)):
        ag_ops[k] = remote(xbuf.at[pl.ds(*src)], xbuf.at[pl.ds(*dst)], ag_s.at[k], ag_r.at[k], to)

    def row_of(t):
        return wrap(y + t)

    def sa_op(t, d):
        dx, h = row_peers[d]
        r = row_of(t)
        return remote(st.at[r, pl.ds(0, 3)], rowa.at[t, 2 * x + c], sa_s.at[t, d], sa_r.at[t, d],
                      dev(y, x + dx, other(h)))

    def sa_wait(t, d):
        dx, h = row_peers[d]
        slot = 2 * wrap(x - dx) + other(h)
        remote(rowa.at[t, slot], rowa.at[t, slot], sa_s.at[t, d], sa_r.at[t, d], partner).wait_recv()

    def sb_op(t, dy):
        r = row_of(t)
        return remote(rowb.at[r, y], rowb.at[r, y], sb_s.at[t, dy], sb_r.at[t, dy], dev(y + dy, x, c))

    def sb_wait(t, dy):
        yy = wrap(y - dy)
        ref = rowb.at[wrap(yy + t), yy]
        remote(ref, ref, sb_s.at[t, dy], sb_r.at[t, dy], partner).wait_recv()

    def merge(parts):
        m = functools.reduce(jnp.maximum, [p[0] for p in parts])
        s = functools.reduce(jnp.add, [p[1] * jnp.exp(p[0] - m) for p in parts])
        return m, s, functools.reduce(jnp.add, [p[2] for p in parts])

    def row_merge(t):
        for d in range(len(row_peers)):
            sa_wait(t, d)
        m, s, q = merge([[rowa[t, i, k] for k in range(3)] for i in range(n_row)])
        r = row_of(t)
        rowb[r, y, 0] = m
        rowb[r, y, 1] = s
        rowb[r, y, 2] = q
        for dy in range(1, side):
            sb_op(t, dy).start()

    half = (vocab // LANES // 2) * LANES
    digit = jnp.where(lane == 0, 1.0, jnp.where(lane == 1, 256.0, jnp.where(lane == 2, 65536.0, 0.0)))

    def logits_tile(t, carry):
        @pl.when(t == 1)
        def _():
            ag_ops[16].wait_recv()

        @pl.when(t == 2)
        def _():
            ag_ops[20].wait_recv()

        @pl.when(t == 3)
        def _():
            ag_ops[17].wait_recv()

        base = 8 * t
        for p in range(8):
            code = jnp.sum(xbuf[base + p, :, dim:wide].astype(F32) * digit, axis=1, keepdims=True)
            tcol[base + p] = jnp.broadcast_to(code.astype(jnp.int32) - 1 - off, (tok, LANES))
        ms[...] = jnp.full(ms.shape, LOW, F32)
        ss[...] = jnp.zeros(ss.shape, F32)
        pk[...] = jnp.zeros(pk.shape, F32)

        def do_dot(o, n):
            xt = xbuf[pl.ds(base, 8), :, 0:dim].reshape(8 * tok, dim)
            r = dot(xt, emb[o:o + n, :], NT) + bias_ref[:, o:o + n]
            z[pl.ds(base, 8), :, o:o + n] = r.reshape(8, tok, n)

        def do_stats(o, n):
            for p in range(8):
                m0, tl, q = ms[p], tcol[base + p], pk[p]
                zs = [z[base + p, :, o + i:o + i + LANES] for i in range(0, n, LANES)]
                m1 = functools.reduce(jnp.maximum, zs, m0)
                s = ss[p] * jnp.exp(m0 - m1)
                for i, v in enumerate(zs):
                    s = s + jnp.exp(v - m1)
                    q = q + jnp.where(lane + (o + i * LANES) == tl, v, 0.0)
                ms[p], ss[p], pk[p] = m1, s, q

        def run(lo_, hi_):
            cs = pieces(lo_, hi_, 512)
            do_dot(*cs[0])
            for a, b in zip(cs[1:], cs[:-1]):
                do_dot(*a)
                do_stats(*b)
            do_stats(*cs[-1])

        run(0, half)

        @pl.when(t == 0)
        def _():
            for k in (3, 9, 11, 14):
                ag_ops[k].wait_recv()
            ag_ops[16].start()
            ag_ops[18].start()
            for k in (4, 10, 12, 15):
                ag_ops[k].wait_recv()
            ag_ops[17].start()
            ag_ops[19].start()

        @pl.when(t == 1)
        def _():
            ag_ops[18].wait_recv()
            ag_ops[19].wait_recv()
            ag_ops[20].start()

        @pl.when(t > 0)
        def _():
            row_merge(t - 1)

        run(half, vocab)

        r = row_of(t)
        for p in range(8):
            h, j = p // 4, p % 4
            m1 = jnp.max(ms[p], axis=1, keepdims=True)
            s1 = jnp.sum(ss[p] * jnp.exp(ms[p] - m1), axis=1, keepdims=True)
            q1 = jnp.sum(pk[p], axis=1, keepdims=True)
            live = jnp.where(tcol[base + p] == -1 - off, 0.0, 1.0)
            packed = jnp.where(lane == 0, m1, jnp.where(lane == 1, s1, jnp.where(lane == 2, q1, live)))
            flat = jnp.concatenate([packed, jnp.zeros((LANES - tok, LANES), F32)], axis=0).T
            sub = 2 * wrap(x + j) + other(h)
            for k in range(3):
                st[r, k, pl.ds(sub, 1), :] = flat[k:k + 1, :]
            mrow[r, pl.ds(sub, 1), :] = flat[3:4, :]
        for k in range(3):
            rowa[t, 2 * x + c, k] = st[r, k]
        for d in range(len(row_peers)):
            sa_op(t, d).start()
        return carry

    emb_copy.wait()
    lax.fori_loop(0, side, logits_tile, 0)
    row_merge(side - 1)
    for t in range(side):
        for dy in range(1, side):
            sb_wait(t, dy)

    n_tok = jnp.sum(mrow[...])
    inv_n = 1.0 / n_tok
    total = jnp.zeros((n_row, LANES), F32)
    lanes8 = lax.broadcasted_iota(jnp.int32, (n_row, LANES), 1)
    for r in range(side):
        m, s, q = merge([[rowb[r, i, k] for k in range(3)] for i in range(side)])
        lse = m + jnp.log(s)
        lrow[r] = lse
        tl = jnp.where(lanes8 < tok, (lse - q) * mrow[r], 0.0)
        st[r, 3] = tl
        total = total + tl
    loss_ref[...] = st[y, 3, pl.ds(2 * x + c, 1), :]
    mean_ref[...] = jnp.broadcast_to(jnp.sum(total) / n_tok, (1, LANES))

    def blk(k, p):
        h, j = p // 4, p % 4
        cc = other(h)
        yy = wrap(jnp.where(cc == 0, x + j + k, y + j))
        xx = wrap(jnp.where(cc == 0, x + j, y + j - k))
        pos = 8 * wrap(yy - y) + 4 * h + wrap(xx - x)
        return pos, yy, 2 * xx + cc

    along = c
    nxt = dev(y + along, x + 1 - along, c)
    prv = dev(y - along, x - 1 + along, c)
    top, bot = pl.ds(0, tok // 2), pl.ds(tok // 2, tok - tok // 2)

    def s0(k):
        return remote(dxt.at[k, pl.ds(4, 4)], rca.at[k], s0_s.at[k], s0_r.at[k], partner)

    def s1(k, d):
        src = dxt.at[k, 2, top] if d == 0 else dxt.at[k, 2, bot]
        return remote(src, rcb.at[k, d], s1_s.at[k, d], s1_r.at[k, d], prv if d == 0 else nxt)

    def s2(k, d):
        src = dxt.at[k, 1] if d == 0 else dxt.at[k, 3]
        return remote(src, rcd.at[k, d], s2_s.at[k, d], s2_r.at[k, d], nxt if d == 0 else prv)

    def s3_far(k):
        return wrap(jnp.where(c == 0, x + k - y, y - k - x))

    def s3(k):
        i = s3_far(k)
        to = dev(jnp.where(c == 0, x + k, y), jnp.where(c == 0, x, y - k), c)
        slot = wrap(side - i)
        return remote(dxt.at[k, 0], rcc.at[slot], s3_s.at[k], s3_r.at[slot], to)

    def do_s1(k):
        s0(k).wait_recv()
        for j in range(4):
            dxt[k, j] = dxt[k, j] + rca[k, j]
        s1(k, 0).start()
        s1(k, 1).start()

    def do_s2(k):
        s1(k, 0).wait_recv()
        s1(k, 1).wait_recv()
        n = tok // 2
        dxt[k, 3, 0:n] = dxt[k, 3, 0:n] + rcb[k, 0]
        dxt[k, 1, n:tok] = dxt[k, 1, n:tok] + rcb[k, 1]
        s2(k, 0).start()
        s2(k, 1).start()

    def do_s3(k):
        s2(k, 0).wait_recv()
        s2(k, 1).wait_recv()
        dxt[k, 0] = dxt[k, 0] + rcd[k, 0] + rcd[k, 1]
        i = s3_far(k)

        @pl.when(i != 0)
        def _():
            s3(k).start()

        @pl.when(i == 0)
        def _():
            rcc[0] = dxt[k, 0]

    def dz_out(k):
        return pltpu.make_async_copy(
            stage.at[lax.rem(k, 2)], dz_hbm.at[pl.ds(pl.multiple_of(k * 8 * tok, 8 * tok), 8 * tok)], dz_sem.at[k])

    def x_out(k, p):
        pos, _, _ = blk(k, p)
        return pltpu.make_async_copy(
            xbuf.at[pos, :, pl.ds(0, dim)],
            x_hbm.at[pl.ds(pl.multiple_of((8 * k + p) * tok, 16), tok)], x_sem.at[8 * k + p])

    def grad_tile(k, carry):
        where = [blk(k, p) for p in range(8)]
        for p, (pos, yy, sub) in enumerate(where):
            row = lrow[yy, pl.ds(sub, 1), :]
            lsec[p] = jnp.broadcast_to(row, (LANES, LANES)).T[0:tok, :]
            wcol[p] = jnp.where(tcol[pos] == -1 - off, 0.0, inv_n)
            x_out(k, p).start()
        buf = lax.rem(k, 2)

        @pl.when(k >= 2)
        def _():
            dz_out(k - 2).wait()

        def part(o, n):
            rows = []
            for p, (pos, _, _) in enumerate(where):
                l, w, tl = lsec[p], wcol[p], tcol[pos]
                cols = []
                for i in range(o, o + n, LANES):
                    e = jnp.exp(z[pos, :, i:i + LANES] - l)
                    e = jnp.where(lane + i == tl, e - 1.0, e) * w
                    cols.append(e.astype(BF16))
                rows.append(jnp.concatenate(cols, axis=1))
            dz = jnp.concatenate(rows, axis=0)
            stage[buf, :, o:o + n] = dz
            return dot(dz, emb[o:o + n, :], NN)

        def span(lo_, hi_):
            return functools.reduce(jnp.add, [part(o, n) for o, n in pieces(lo_, hi_, 512)])

        dxt[k] = span(0, half).reshape(8, tok, dim)

        @pl.when(k >= 1)
        def _():
            do_s1(k - 1)

        @pl.when(k >= 2)
        def _():
            do_s2(k - 2)

        @pl.when(k >= 3)
        def _():
            do_s3(k - 3)

        dxt[k] = dxt[k] + span(half, vocab).reshape(8, tok, dim)
        s0(k).start()
        dz_out(k).start()
        return carry

    lax.fori_loop(0, side, grad_tile, 0)
    last = side - 1
    do_s1(last)
    do_s2(last - 1)
    do_s3(last - 2)
    do_s2(last)
    do_s3(last - 1)
    do_s3(last)
    for i in range(1, side):
        ref = rcc.at[i]
        remote(ref, ref, s3_s.at[0], s3_r.at[i], partner).wait_recv()

    dx = rcc[0] + rcc[1] + rcc[2] + rcc[3]
    xhat, rstd = normed()
    g = dx * gamma_ref[...][None, :]
    dh = rstd * (g - jnp.mean(g, axis=-1, keepdims=True) - xhat * jnp.mean(g * xhat, axis=-1, keepdims=True))
    gpart[0:1, :] = jnp.sum(dx * xhat, axis=0, keepdims=True)
    gpart[1:2, :] = jnp.sum(dx, axis=0, keepdims=True)

    def ga_op(d):
        ddx, h = row_peers[d]
        return remote(gpart, ga.at[2 * x + c], ga_s.at[d], ga_r.at[d], dev(y, x + ddx, other(h)))

    def gb_op(dy):
        return remote(gb.at[y], gb.at[y], gb_s.at[dy], gb_r.at[dy], dev(y + dy, x, c))

    for d in range(len(row_peers)):
        ga_op(d).start()
    dhid_ref[...] = dh.astype(BF16)
    ga[2 * x + c] = gpart[...]
    for d, (ddx, h) in enumerate(row_peers):
        ref = ga.at[2 * wrap(x - ddx) + other(h)]
        remote(ref, ref, ga_s.at[d], ga_r.at[d], partner).wait_recv()
    gb[y] = functools.reduce(jnp.add, [ga[i] for i in range(n_row)])
    for dy in range(1, side):
        gb_op(dy).start()
    for dy in range(1, side):
        ref = gb.at[wrap(y - dy)]
        remote(ref, ref, gb_s.at[dy], gb_r.at[dy], partner).wait_recv()
    dln_ref[...] = functools.reduce(jnp.add, [gb[i] for i in range(side)])

    for k in sorted(ag_ops):
        ag_ops[k].wait_send()
    for t in range(side):
        for d in range(len(row_peers)):
            sa_op(t, d).wait_send()
        for dy in range(1, side):
            sb_op(t, dy).wait_send()
        s0(t).wait_send()
        for d in range(2):
            s1(t, d).wait_send()
            s2(t, d).wait_send()

        @pl.when(s3_far(t) != 0)
        def _():
            s3(t).wait_send()

        for p in range(8):
            x_out(t, p).wait()
    for d in range(len(row_peers)):
        ga_op(d).wait_send()
    for dy in range(1, side):
        gb_op(dy).wait_send()
    dz_out(side - 2).wait()
    dz_out(side - 1).wait()


def head(mesh, hid, gamma, beta, valid, tgt, mask, emb):
    n_dev = mesh.shape["tp"]
    side = math.isqrt(n_dev // 2)
    tok, dim = hid.shape
    vocab = emb.shape[0]
    seq = tok * n_dev
    n_row = 2 * side
    vmem = pl.BlockSpec(memory_space=pltpu.VMEM)
    hbm = pl.BlockSpec(memory_space=pl.ANY)
    dma = pltpu.SemaphoreType.DMA
    return pl.pallas_call(
        functools.partial(head_kernel, side, tok, dim, vocab),
        out_shape=(
            jax.ShapeDtypeStruct((1, LANES), F32),
            jax.ShapeDtypeStruct((1, LANES), F32),
            jax.ShapeDtypeStruct((tok, dim), BF16),
            jax.ShapeDtypeStruct((2, dim), F32),
            jax.ShapeDtypeStruct((seq, vocab), BF16),
            jax.ShapeDtypeStruct((seq, dim), BF16),
        ),
        in_specs=[vmem] * 6 + [hbm],
        out_specs=(vmem, vmem, vmem, vmem, hbm, hbm),
        scratch_shapes=[
            pltpu.VMEM((vocab, dim), BF16),
            pltpu.VMEM((n_dev, tok, dim + LANES), BF16),
            pltpu.VMEM((n_dev, tok, vocab), F32),
            pltpu.VMEM((1, vocab), F32),
            pltpu.VMEM((1, LANES), F32),
            pltpu.VMEM((n_dev, tok, LANES), jnp.int32),
            pltpu.VMEM((2, 8 * tok, vocab), BF16),
            pltpu.VMEM((8, tok, LANES), F32),
            pltpu.VMEM((8, tok, LANES), F32),
            pltpu.VMEM((8, tok, LANES), F32),
            pltpu.VMEM((8, tok, LANES), F32),
            pltpu.VMEM((8, tok, LANES), F32),
            pltpu.VMEM((side, 4, n_row, LANES), F32),
            pltpu.VMEM((side, n_row, 3, n_row, LANES), F32),
            pltpu.VMEM((side, side, 3, n_row, LANES), F32),
            pltpu.VMEM((side, n_row, LANES), F32),
            pltpu.VMEM((side, n_row, LANES), F32),
            pltpu.VMEM((side, 8, tok, dim), F32),
            pltpu.VMEM((side, 4, tok, dim), F32),
            pltpu.VMEM((side, 2, tok // 2, dim), F32),
            pltpu.VMEM((side, 2, tok, dim), F32),
            pltpu.VMEM((side, tok, dim), F32),
            pltpu.VMEM((n_row, 2, dim), F32),
            pltpu.VMEM((side, 2, dim), F32),
            pltpu.VMEM((2, dim), F32),
            dma,
            dma((21,)), dma((21,)),
            dma((side, n_row - 1)), dma((side, n_row - 1)),
            dma((side, side)), dma((side, side)),
            dma((side,)), dma((side,)),
            dma((side, 2)), dma((side, 2)),
            dma((side, 2)), dma((side, 2)),
            dma((side,)), dma((side,)),
            dma((n_row - 1,)), dma((n_row - 1,)),
            dma((side,)), dma((side,)),
            dma((side,)), dma((n_dev,)),
        ],
        compiler_params=pltpu.CompilerParams(
            collective_id=0, has_side_effects=True, vmem_limit_bytes=67043328),
        name="head",
    )(hid, gamma, beta, valid, tgt, mask, emb)


def dembed_kernel(x_ref, dz_ref, loss_in, mean_in, dhid_in, dln_in, out_ref, loss_ref, mean_ref, dhid_ref, dln_ref):
    out_ref[...] = dot(dz_ref[...], x_ref[...], TN)

    @pl.when(pl.program_id(0) == 0)
    def _():
        loss_ref[...] = loss_in[...]
        mean_ref[...] = mean_in[...]
        dhid_ref[...] = dhid_in[...]
        dln_ref[...] = dln_in[...]


def dembed(x, dz, loss, mean, dhid, dln):
    seq, dim = x.shape
    vocab = dz.shape[1]
    cols = 1664
    small = [pl.BlockSpec(v.shape, lambda i: (0, 0)) for v in (loss, mean, dhid, dln)]
    return pl.pallas_call(
        dembed_kernel,
        out_shape=(jax.ShapeDtypeStruct((vocab, dim), F32),)
        + tuple(jax.ShapeDtypeStruct(v.shape, v.dtype) for v in (loss, mean, dhid, dln)),
        grid=(pl.cdiv(vocab, cols),),
        in_specs=[pl.BlockSpec((seq, dim), lambda i: (0, 0)), pl.BlockSpec((seq, cols), lambda i: (0, i))] + small,
        out_specs=tuple([pl.BlockSpec((cols, dim), lambda i: (i, 0))] + small),
        compiler_params=pltpu.CompilerParams(vmem_limit_bytes=67043328),
        name="dembed",
    )(x, dz, loss, mean, dhid, dln)


def solution(mesh):
    tok_spec = P(("dp", "tp"))
    row_spec = P(("dp", "tp"), None)

    def local_step(hidden_blk, ln_gamma, ln_beta, embed_blk, valid_blk, tgt_blk, mask_blk):
        loss, mean, dhid, dln, dz, x = head(
            mesh, hidden_blk, ln_gamma, ln_beta, valid_blk, tgt_blk, mask_blk, embed_blk)
        d_embed, loss, mean, d_hidden, dln = dembed(x, dz, loss, mean, dhid, dln)
        return loss[0, :dhid.shape[0]], mean[0, :1], d_hidden, d_embed, dln[0], dln[1]

    return jax.shard_map(
        local_step, mesh=mesh,
        in_specs=(row_spec, P(), P(), P("tp", None), P("tp"), tok_spec, tok_spec),
        out_specs=(tok_spec, P("dp"), row_spec, row_spec, P("dp"), P("dp")), check_vma=False)
```

```python
import functools
import math

import jax
import jax.numpy as jnp
from jax import lax
from jax.experimental import pallas as pl
from jax.experimental.pallas import tpu as pltpu
from jax.sharding import PartitionSpec as P

LN_EPS = 1e-5
F32 = jnp.float32
BF16 = jnp.bfloat16
LANES = 128
LOW = -3e38
NN = (((1,), (0,)), ((), ()))
NT = (((1,), (1,)), ((), ()))
TN = (((0,), (0,)), ((), ()))


def dot(a, b, dims):
    return lax.dot_general(a, b, dims, preferred_element_type=F32)


def pieces(lo, hi, size):
    return [(o, min(size, hi - o)) for o in range(lo, hi, size)]


def head_kernel(
    side, tok, dim, vocab,
    hid_ref, gamma_ref, beta_ref, valid_ref, tgt_ref, mask_ref, emb_hbm,
    loss_ref, mean_ref, dhid_ref, dgam_ref, dbet_ref, dz_hbm, x_hbm,
    emb, xbuf, z, bias_ref, crow, tcol, stage, ms, ss, pk, lsec, wcol,
    st, rowa, rowb, mrow, lrow,
    dxt, rca, rcb, rcd, rcc, ga, gb, gpart,
    emb_sem, ag_s, ag_r, sa_s, sa_r, sb_s, sb_r,
    s0_s, s0_r, s1_s, s1_r, s2_s, s2_r, s3_s, s3_r,
    ga_s, ga_r, gb_s, gb_r, dz_sem, x_sem,
):
    n_row = 2 * side
    wide = dim + LANES
    me = lax.axis_index("tp")
    c = lax.rem(me, 2)
    x = lax.rem(me // 2, side)
    y = me // n_row
    off = me * vocab

    def wrap(v):
        return lax.rem(v + 4 * side, side)

    def dev(yy, xx, cc):
        return {"tp": (wrap(yy) * side + wrap(xx)) * 2 + cc}

    right, left = dev(y, x + 1, c), dev(y, x - 1, c)
    up, down = dev(y - 1, x, c), dev(y + 1, x, c)
    partner = dev(y, x, 1 - c)
    row_peers = [(dx, h) for h in range(2) for dx in range(side) if (dx, h) != (0, 0)]

    def other(h):
        return c if h == 0 else 1 - c

    def remote(src, dst, s, r, to):
        return pltpu.make_async_remote_copy(
            src_ref=src, dst_ref=dst, send_sem=s, recv_sem=r,
            device_id=to, device_id_type=pl.DeviceIdType.MESH)

    emb_copy = pltpu.make_async_copy(emb_hbm, emb, emb_sem)
    emb_copy.start()

    barrier = pltpu.get_barrier_semaphore()
    for dx, h in row_peers:
        pl.semaphore_signal(barrier, inc=1, device_id=dev(y, x + dx, other(h)),
                            device_id_type=pl.DeviceIdType.MESH)
    for dy in range(1, side):
        pl.semaphore_signal(barrier, inc=1, device_id=dev(y + dy, x, c),
                            device_id_type=pl.DeviceIdType.MESH)

    def normed():
        h32 = hid_ref[...].astype(F32)
        cen = h32 - jnp.mean(h32, axis=-1, keepdims=True)
        rstd = lax.rsqrt(jnp.mean(cen * cen, axis=-1, keepdims=True) + LN_EPS)
        return cen * rstd, rstd

    xhat0, _ = normed()
    xbuf[0, :, 0:dim] = (xhat0 * gamma_ref[...][None, :] + beta_ref[...][None, :]).astype(BF16)
    crow[...] = jnp.zeros((1, LANES), F32)
    crow[0:1, 0:tok] = jnp.where(mask_ref[...] > 0, tgt_ref[...] + 1, 0).astype(F32)[None, :]
    lane = lax.broadcasted_iota(jnp.int32, (tok, LANES), 1)
    ccol = jnp.broadcast_to(crow[...], (LANES, LANES)).T[0:tok, :].astype(jnp.int32)
    digits = jnp.where(lane == 0, ccol & 255, jnp.where(lane == 1, (ccol >> 8) & 255, (ccol >> 16) & 255))
    xbuf[0, :, dim:wide] = jnp.where(lane < 3, digits, 0).astype(F32).astype(BF16)
    pl.semaphore_wait(barrier, len(row_peers) + side - 1)

    bias_ref[...] = jnp.where(valid_ref[...] > 0, 0.0, -jnp.inf).astype(F32)[None, :]

    cut = 2 * tok // 3
    lo, hi = pl.ds(0, cut), pl.ds(cut, tok - cut)
    ag_ops = {}

    def ag(k, src, dst, to, rows=None):
        a, b = xbuf.at[src], xbuf.at[dst]
        if rows is not None:
            a, b = xbuf.at[src, rows], xbuf.at[dst, rows]
        ag_ops[k] = remote(a, b, ag_s.at[k], ag_r.at[k], to)
        ag_ops[k].start()

    ag(0, 0, 3, right)
    ag(1, 0, 1, left)
    ag(2, 0, 4, partner)
    ag(3, 0, 8, up)
    ag(4, 0, 24, down)
    ag_ops[0].wait_recv()
    ag(5, 3, 2, right, lo)
    ag(7, 3, 7, partner)
    ag(9, 3, 11, up)
    ag(10, 3, 27, down)
    ag_ops[1].wait_recv()
    ag(6, 1, 2, left, hi)
    ag(8, 1, 5, partner)
    ag(11, 1, 9, up)
    ag(12, 1, 25, down)
    ag_ops[5].wait_recv()
    ag_ops[6].wait_recv()
    ag(13, 2, 6, partner)
    ag(14, 2, 10, up)
    ag(15, 2, 26, down)
    for k in (2, 7, 8, 13):
        ag_ops[k].wait_recv()
    for k, src, dst, to in ((16, (8, 4), (12, 4), partner), (17, (24, 4), (28, 4), partner),
                            (18, (8, 2), (16, 2), up), (19, (26, 2), (18, 2), down),
                            (20, (16, 4), (20, 4), partner)):
        ag_ops[k] = remote(xbuf.at[pl.ds(*src)], xbuf.at[pl.ds(*dst)], ag_s.at[k], ag_r.at[k], to)

    def row_of(t):
        return wrap(y + t)

    def sa_op(t, d):
        dx, h = row_peers[d]
        r = row_of(t)
        return remote(st.at[r, pl.ds(0, 3)], rowa.at[t, 2 * x + c], sa_s.at[t, d], sa_r.at[t, d],
                      dev(y, x + dx, other(h)))

    def sa_wait(t, d):
        dx, h = row_peers[d]
        slot = 2 * wrap(x - dx) + other(h)
        remote(rowa.at[t, slot], rowa.at[t, slot], sa_s.at[t, d], sa_r.at[t, d], partner).wait_recv()

    def sb_op(t, dy):
        r = row_of(t)
        return remote(rowb.at[r, y], rowb.at[r, y], sb_s.at[t, dy], sb_r.at[t, dy], dev(y + dy, x, c))

    def sb_wait(t, dy):
        yy = wrap(y - dy)
        ref = rowb.at[wrap(yy + t), yy]
        remote(ref, ref, sb_s.at[t, dy], sb_r.at[t, dy], partner).wait_recv()

    def merge(parts):
        m = functools.reduce(jnp.maximum, [p[0] for p in parts])
        s = functools.reduce(jnp.add, [p[1] * jnp.exp(p[0] - m) for p in parts])
        return m, s, functools.reduce(jnp.add, [p[2] for p in parts])

    def row_merge(t):
        for d in range(len(row_peers)):
            sa_wait(t, d)
        m, s, q = merge([[rowa[t, i, k] for k in range(3)] for i in range(n_row)])
        r = row_of(t)
        rowb[r, y, 0] = m
        rowb[r, y, 1] = s
        rowb[r, y, 2] = q
        for dy in range(1, side):
            sb_op(t, dy).start()

    half = (vocab // LANES // 2) * LANES
    digit = jnp.where(lane == 0, 1.0, jnp.where(lane == 1, 256.0, jnp.where(lane == 2, 65536.0, 0.0)))

    def logits_tile(t, carry):
        @pl.when(t == 1)
        def _():
            ag_ops[16].wait_recv()

        @pl.when(t == 2)
        def _():
            ag_ops[20].wait_recv()

        @pl.when(t == 3)
        def _():
            ag_ops[17].wait_recv()

        base = 8 * t
        for p in range(8):
            code = jnp.sum(xbuf[base + p, :, dim:wide].astype(F32) * digit, axis=1, keepdims=True)
            tcol[base + p] = jnp.broadcast_to(code.astype(jnp.int32) - 1 - off, (tok, LANES))
        ms[...] = jnp.full(ms.shape, LOW, F32)
        ss[...] = jnp.zeros(ss.shape, F32)
        pk[...] = jnp.zeros(pk.shape, F32)

        def do_dot(o, n):
            xt = xbuf[pl.ds(base, 8), :, 0:dim].reshape(8 * tok, dim)
            r = dot(xt, emb[o:o + n, :], NT) + bias_ref[:, o:o + n]
            z[pl.ds(base, 8), :, o:o + n] = r.reshape(8, tok, n)

        def do_stats(o, n):
            for p in range(8):
                m0, tl, q = ms[p], tcol[base + p], pk[p]
                zs = [z[base + p, :, o + i:o + i + LANES] for i in range(0, n, LANES)]
                m1 = functools.reduce(jnp.maximum, zs, m0)
                s = ss[p] * jnp.exp(m0 - m1)
                for i, v in enumerate(zs):
                    s = s + jnp.exp(v - m1)
                    q = q + jnp.where(lane + (o + i * LANES) == tl, v, 0.0)
                ms[p], ss[p], pk[p] = m1, s, q

        def run(lo_, hi_):
            cs = pieces(lo_, hi_, 512)
            do_dot(*cs[0])
            for a, b in zip(cs[1:], cs[:-1]):
                do_dot(*a)
                do_stats(*b)
            do_stats(*cs[-1])

        run(0, half)

        @pl.when(t == 0)
        def _():
            for k in (3, 9, 11, 14):
                ag_ops[k].wait_recv()
            ag_ops[16].start()
            ag_ops[18].start()
            for k in (4, 10, 12, 15):
                ag_ops[k].wait_recv()
            ag_ops[17].start()
            ag_ops[19].start()

        @pl.when(t == 1)
        def _():
            ag_ops[18].wait_recv()
            ag_ops[19].wait_recv()
            ag_ops[20].start()

        @pl.when(t > 0)
        def _():
            row_merge(t - 1)

        run(half, vocab)

        r = row_of(t)
        for p in range(8):
            h, j = p // 4, p % 4
            m1 = jnp.max(ms[p], axis=1, keepdims=True)
            s1 = jnp.sum(ss[p] * jnp.exp(ms[p] - m1), axis=1, keepdims=True)
            q1 = jnp.sum(pk[p], axis=1, keepdims=True)
            live = jnp.where(tcol[base + p] == -1 - off, 0.0, 1.0)
            packed = jnp.where(lane == 0, m1, jnp.where(lane == 1, s1, jnp.where(lane == 2, q1, live)))
            flat = jnp.concatenate([packed, jnp.zeros((LANES - tok, LANES), F32)], axis=0).T
            sub = 2 * wrap(x + j) + other(h)
            for k in range(3):
                st[r, k, pl.ds(sub, 1), :] = flat[k:k + 1, :]
            mrow[r, pl.ds(sub, 1), :] = flat[3:4, :]
        for k in range(3):
            rowa[t, 2 * x + c, k] = st[r, k]
        for d in range(len(row_peers)):
            sa_op(t, d).start()
        return carry

    emb_copy.wait()
    lax.fori_loop(0, side, logits_tile, 0)
    row_merge(side - 1)
    for t in range(side):
        for dy in range(1, side):
            sb_wait(t, dy)

    n_tok = jnp.sum(mrow[...])
    inv_n = 1.0 / n_tok
    total = jnp.zeros((n_row, LANES), F32)
    lanes8 = lax.broadcasted_iota(jnp.int32, (n_row, LANES), 1)
    for r in range(side):
        m, s, q = merge([[rowb[r, i, k] for k in range(3)] for i in range(side)])
        lse = m + jnp.log(s)
        lrow[r] = lse
        tl = jnp.where(lanes8 < tok, (lse - q) * mrow[r], 0.0)
        st[r, 3] = tl
        total = total + tl
    loss_ref[...] = st[y, 3, pl.ds(2 * x + c, 1), :]
    mean_ref[...] = jnp.broadcast_to(jnp.sum(total) / n_tok, (1, LANES))

    def blk(k, p):
        h, j = p // 4, p % 4
        cc = other(h)
        yy = wrap(jnp.where(cc == 0, x + j + k, y + j))
        xx = wrap(jnp.where(cc == 0, x + j, y + j - k))
        pos = 8 * wrap(yy - y) + 4 * h + wrap(xx - x)
        return pos, yy, 2 * xx + cc

    along = c
    nxt = dev(y + along, x + 1 - along, c)
    prv = dev(y - along, x - 1 + along, c)
    top, bot = pl.ds(0, tok // 2), pl.ds(tok // 2, tok - tok // 2)

    def s0(k):
        return remote(dxt.at[k, pl.ds(4, 4)], rca.at[k], s0_s.at[k], s0_r.at[k], partner)

    def s1(k, d):
        src = dxt.at[k, 2, top] if d == 0 else dxt.at[k, 2, bot]
        return remote(src, rcb.at[k, d], s1_s.at[k, d], s1_r.at[k, d], prv if d == 0 else nxt)

    def s2(k, d):
        src = dxt.at[k, 1] if d == 0 else dxt.at[k, 3]
        return remote(src, rcd.at[k, d], s2_s.at[k, d], s2_r.at[k, d], nxt if d == 0 else prv)

    def s3_far(k):
        return wrap(jnp.where(c == 0, x + k - y, y - k - x))

    def s3(k):
        i = s3_far(k)
        to = dev(jnp.where(c == 0, x + k, y), jnp.where(c == 0, x, y - k), c)
        slot = wrap(side - i)
        return remote(dxt.at[k, 0], rcc.at[slot], s3_s.at[k], s3_r.at[slot], to)

    def do_s1(k):
        s0(k).wait_recv()
        for j in range(4):
            dxt[k, j] = dxt[k, j] + rca[k, j]
        s1(k, 0).start()
        s1(k, 1).start()

    def do_s2(k):
        s1(k, 0).wait_recv()
        s1(k, 1).wait_recv()
        n = tok // 2
        dxt[k, 3, 0:n] = dxt[k, 3, 0:n] + rcb[k, 0]
        dxt[k, 1, n:tok] = dxt[k, 1, n:tok] + rcb[k, 1]
        s2(k, 0).start()
        s2(k, 1).start()

    def do_s3(k):
        s2(k, 0).wait_recv()
        s2(k, 1).wait_recv()
        dxt[k, 0] = dxt[k, 0] + rcd[k, 0] + rcd[k, 1]
        i = s3_far(k)

        @pl.when(i != 0)
        def _():
            s3(k).start()

        @pl.when(i == 0)
        def _():
            rcc[0] = dxt[k, 0]

    def dz_out(k):
        return pltpu.make_async_copy(
            stage.at[lax.rem(k, 2)], dz_hbm.at[pl.ds(pl.multiple_of(k * 8 * tok, 8 * tok), 8 * tok)], dz_sem.at[k])

    def x_out(k, p):
        pos, _, _ = blk(k, p)
        return pltpu.make_async_copy(
            xbuf.at[pos, :, pl.ds(0, dim)],
            x_hbm.at[pl.ds(pl.multiple_of((8 * k + p) * tok, 16), tok)], x_sem.at[8 * k + p])

    def grad_tile(k, carry):
        where = [blk(k, p) for p in range(8)]
        for p, (pos, yy, sub) in enumerate(where):
            row = lrow[yy, pl.ds(sub, 1), :]
            lsec[p] = jnp.broadcast_to(row, (LANES, LANES)).T[0:tok, :]
            wcol[p] = jnp.where(tcol[pos] == -1 - off, 0.0, inv_n)
            x_out(k, p).start()
        buf = lax.rem(k, 2)

        @pl.when(k >= 2)
        def _():
            dz_out(k - 2).wait()

        def part(o, n):
            rows = []
            for p, (pos, _, _) in enumerate(where):
                l, w, tl = lsec[p], wcol[p], tcol[pos]
                cols = []
                for i in range(o, o + n, LANES):
                    e = jnp.exp(z[pos, :, i:i + LANES] - l)
                    e = jnp.where(lane + i == tl, e - 1.0, e) * w
                    cols.append(e.astype(BF16))
                rows.append(jnp.concatenate(cols, axis=1))
            dz = jnp.concatenate(rows, axis=0)
            stage[buf, :, o:o + n] = dz
            return dot(dz, emb[o:o + n, :], NN)

        def span(lo_, hi_):
            return functools.reduce(jnp.add, [part(o, n) for o, n in pieces(lo_, hi_, 512)])

        dxt[k] = span(0, half).reshape(8, tok, dim)

        @pl.when(k >= 1)
        def _():
            do_s1(k - 1)

        @pl.when(k >= 2)
        def _():
            do_s2(k - 2)

        @pl.when(k >= 3)
        def _():
            do_s3(k - 3)

        dxt[k] = dxt[k] + span(half, vocab).reshape(8, tok, dim)
        s0(k).start()
        dz_out(k).start()
        return carry

    lax.fori_loop(0, side, grad_tile, 0)
    last = side - 1
    do_s1(last)
    do_s2(last - 1)
    do_s3(last - 2)
    do_s2(last)
    do_s3(last - 1)
    do_s3(last)
    for i in range(1, side):
        ref = rcc.at[i]
        remote(ref, ref, s3_s.at[0], s3_r.at[i], partner).wait_recv()

    dx = rcc[0] + rcc[1] + rcc[2] + rcc[3]
    xhat, rstd = normed()
    g = dx * gamma_ref[...][None, :]
    dh = rstd * (g - jnp.mean(g, axis=-1, keepdims=True) - xhat * jnp.mean(g * xhat, axis=-1, keepdims=True))
    gpart[0:1, :] = jnp.sum(dx * xhat, axis=0, keepdims=True)
    gpart[1:2, :] = jnp.sum(dx, axis=0, keepdims=True)

    def ga_op(d):
        ddx, h = row_peers[d]
        return remote(gpart, ga.at[2 * x + c], ga_s.at[d], ga_r.at[d], dev(y, x + ddx, other(h)))

    def gb_op(dy):
        return remote(gb.at[y], gb.at[y], gb_s.at[dy], gb_r.at[dy], dev(y + dy, x, c))

    for d in range(len(row_peers)):
        ga_op(d).start()
    dhid_ref[...] = dh.astype(BF16)
    ga[2 * x + c] = gpart[...]
    for d, (ddx, h) in enumerate(row_peers):
        ref = ga.at[2 * wrap(x - ddx) + other(h)]
        remote(ref, ref, ga_s.at[d], ga_r.at[d], partner).wait_recv()
    gb[y] = functools.reduce(jnp.add, [ga[i] for i in range(n_row)])
    for dy in range(1, side):
        gb_op(dy).start()
    for dy in range(1, side):
        ref = gb.at[wrap(y - dy)]
        remote(ref, ref, gb_s.at[dy], gb_r.at[dy], partner).wait_recv()
    dln = functools.reduce(jnp.add, [gb[i] for i in range(side)])
    dgam_ref[...] = dln[0:1, :]
    dbet_ref[...] = dln[1:2, :]

    for k in sorted(ag_ops):
        ag_ops[k].wait_send()
    for t in range(side):
        for d in range(len(row_peers)):
            sa_op(t, d).wait_send()
        for dy in range(1, side):
            sb_op(t, dy).wait_send()
        s0(t).wait_send()
        for d in range(2):
            s1(t, d).wait_send()
            s2(t, d).wait_send()

        @pl.when(s3_far(t) != 0)
        def _():
            s3(t).wait_send()

        for p in range(8):
            x_out(t, p).wait()
    for d in range(len(row_peers)):
        ga_op(d).wait_send()
    for dy in range(1, side):
        gb_op(dy).wait_send()
    dz_out(side - 2).wait()
    dz_out(side - 1).wait()


def head(mesh, hid, gamma, beta, valid, tgt, mask, emb):
    n_dev = mesh.shape["tp"]
    side = math.isqrt(n_dev // 2)
    tok, dim = hid.shape
    vocab = emb.shape[0]
    seq = tok * n_dev
    n_row = 2 * side
    vmem = pl.BlockSpec(memory_space=pltpu.VMEM)
    hbm = pl.BlockSpec(memory_space=pl.ANY)
    dma = pltpu.SemaphoreType.DMA
    return pl.pallas_call(
        functools.partial(head_kernel, side, tok, dim, vocab),
        out_shape=(
            jax.ShapeDtypeStruct((1, LANES), F32),
            jax.ShapeDtypeStruct((1, LANES), F32),
            jax.ShapeDtypeStruct((tok, dim), BF16),
            jax.ShapeDtypeStruct((1, dim), F32),
            jax.ShapeDtypeStruct((1, dim), F32),
            jax.ShapeDtypeStruct((seq, vocab), BF16),
            jax.ShapeDtypeStruct((seq, dim), BF16),
        ),
        in_specs=[vmem] * 6 + [hbm],
        out_specs=(vmem, vmem, vmem, vmem, vmem, hbm, hbm),
        scratch_shapes=[
            pltpu.VMEM((vocab, dim), BF16),
            pltpu.VMEM((n_dev, tok, dim + LANES), BF16),
            pltpu.VMEM((n_dev, tok, vocab), F32),
            pltpu.VMEM((1, vocab), F32),
            pltpu.VMEM((1, LANES), F32),
            pltpu.VMEM((n_dev, tok, LANES), jnp.int32),
            pltpu.VMEM((2, 8 * tok, vocab), BF16),
            pltpu.VMEM((8, tok, LANES), F32),
            pltpu.VMEM((8, tok, LANES), F32),
            pltpu.VMEM((8, tok, LANES), F32),
            pltpu.VMEM((8, tok, LANES), F32),
            pltpu.VMEM((8, tok, LANES), F32),
            pltpu.VMEM((side, 4, n_row, LANES), F32),
            pltpu.VMEM((side, n_row, 3, n_row, LANES), F32),
            pltpu.VMEM((side, side, 3, n_row, LANES), F32),
            pltpu.VMEM((side, n_row, LANES), F32),
            pltpu.VMEM((side, n_row, LANES), F32),
            pltpu.VMEM((side, 8, tok, dim), F32),
            pltpu.VMEM((side, 4, tok, dim), F32),
            pltpu.VMEM((side, 2, tok // 2, dim), F32),
            pltpu.VMEM((side, 2, tok, dim), F32),
            pltpu.VMEM((side, tok, dim), F32),
            pltpu.VMEM((n_row, 2, dim), F32),
            pltpu.VMEM((side, 2, dim), F32),
            pltpu.VMEM((2, dim), F32),
            dma,
            dma((21,)), dma((21,)),
            dma((side, n_row - 1)), dma((side, n_row - 1)),
            dma((side, side)), dma((side, side)),
            dma((side,)), dma((side,)),
            dma((side, 2)), dma((side, 2)),
            dma((side, 2)), dma((side, 2)),
            dma((side,)), dma((side,)),
            dma((n_row - 1,)), dma((n_row - 1,)),
            dma((side,)), dma((side,)),
            dma((side,)), dma((n_dev,)),
        ],
        compiler_params=pltpu.CompilerParams(
            collective_id=0, has_side_effects=True, vmem_limit_bytes=67043328),
        name="head",
    )(hid, gamma, beta, valid, tgt, mask, emb)


def dembed_kernel(
    x_ref, dz_ref, loss_in, mean_in, dhid_in, dgam_in, dbet_in,
    out_ref, loss_ref, mean_ref, dhid_ref, dgam_ref, dbet_ref,
):
    out_ref[...] = dot(dz_ref[...], x_ref[...], TN)

    @pl.when(pl.program_id(0) == 0)
    def _():
        loss_ref[...] = loss_in[...]
        mean_ref[...] = mean_in[...]
        dhid_ref[...] = dhid_in[...]
        dgam_ref[...] = dgam_in[0, :]
        dbet_ref[...] = dbet_in[0, :]


def dembed(x, dz, loss, mean, dhid, dgam, dbet):
    seq, dim = x.shape
    vocab = dz.shape[1]
    cols = 1664
    small = [pl.BlockSpec(v.shape, lambda i: (0, 0)) for v in (loss, mean, dhid, dgam, dbet)]
    flat = pl.BlockSpec((dim,), lambda i: (0,))
    return pl.pallas_call(
        dembed_kernel,
        out_shape=(jax.ShapeDtypeStruct((vocab, dim), F32),)
        + tuple(jax.ShapeDtypeStruct(v.shape, v.dtype) for v in (loss, mean, dhid))
        + (jax.ShapeDtypeStruct((dim,), F32),) * 2,
        grid=(pl.cdiv(vocab, cols),),
        in_specs=[pl.BlockSpec((seq, dim), lambda i: (0, 0)), pl.BlockSpec((seq, cols), lambda i: (0, i))] + small,
        out_specs=tuple([pl.BlockSpec((cols, dim), lambda i: (i, 0))] + small[:3] + [flat] * 2),
        compiler_params=pltpu.CompilerParams(vmem_limit_bytes=67043328),
        name="dembed",
    )(x, dz, loss, mean, dhid, dgam, dbet)


def solution(mesh):
    tok_spec = P(("dp", "tp"))
    row_spec = P(("dp", "tp"), None)

    def local_step(hidden_blk, ln_gamma, ln_beta, embed_blk, valid_blk, tgt_blk, mask_blk):
        loss, mean, dhid, dgam, dbet, dz, x = head(
            mesh, hidden_blk, ln_gamma, ln_beta, valid_blk, tgt_blk, mask_blk, embed_blk)
        d_embed, loss, mean, d_hidden, d_gamma, d_beta = dembed(x, dz, loss, mean, dhid, dgam, dbet)
        return loss[0, :dhid.shape[0]], mean[0, :1], d_hidden, d_embed, d_gamma, d_beta

    return jax.shard_map(
        local_step, mesh=mesh,
        in_specs=(row_spec, P(), P(), P("tp", None), P("tp"), tok_spec, tok_spec),
        out_specs=(tok_spec, P("dp"), row_spec, row_spec, P("dp"), P("dp")), check_vma=False)
```
